32 devices in a mesh: groups: 2 (over x), expert: 8 (over z, y), dp: 2 (over core).
Axes of the slice: x: 2, y: 2, z: 4, core: 2. Of those that a mesh axis runs over, the one named last changes fastest.
Arguments:
- tokens: bfloat16 [128, 2880], P(('groups', 'expert', 'dp')), parts along dimension 0, may hold values from -6 to 6
- norm_gain: bfloat16 [2, 2880], replicated, may hold values from 0.25 to 1.75
- w_gate: bfloat16 [2, 2880, 23040], P(None, None, ('expert', 'dp')), may hold values from -0.109375 to 0.109375
- w_up: bfloat16 [2, 2880, 23040], P(None, None, ('expert', 'dp')), may hold values from -0.109375 to 0.109375
- w_down: bfloat16 [2, 23040, 2880], P(None, ('expert', 'dp')), may hold values from -0.109375 to 0.109375
- routes: int32 [2, 128, 4], P(None, ('groups', 'expert', 'dp')), parts along dimension 1, may hold values from 0 to 7, all different within a row; in each aligned block of 4 rows (0 to 3, 4 to 7, ..., all dimensions but the last counted through in order) at most 3 rows name the same one
- gates: float32 [2, 128, 4], P(None, ('groups', 'expert', 'dp')), parts along dimension 1, may hold values from 0.1 to 1
Outputs:
- mixed: bfloat16 [128, 2880], P(('groups', 'expert', 'dp')), parts along dimension 0
The draws below stay inside these ranges and needn't reach their ends.
There are 2 independent parts, one for each index of `groups`. The reference program is written for one: setup_inputs(seed, part) draws one part's arguments, and reference() takes and returns one part's arrays. A program takes and returns all parts, laid end to end along the dimension named above; an argument that names none is the same for every part. Nothing has to cross between parts.
Inputs may be any that keep to these rules, and one draw needn't show every extreme that they name: `routes`: each token names 4 different experts; among the 4 rows of one device (aligned blocks of a layer) no expert is named more than 3 times, and in every layer some device's block names some expert exactly 3 times.
All inputs are finite; a program needn't handle non-finite values.
Results may differ from the reference program's by a relative error of at most 0.014.
Values may be sent and summed in bfloat16 or wider, within the bound.
A program may use at most 128 MiB of HBM per device.

```python
import math
import jax
import jax.numpy as jnp
import numpy as np
from jax import lax

D = 2880
FF = 2880
TOP = 4
LAYERS = 2
TOK_DEV = 4
EXPERTS = 8
CAP = 3
TOKENS = 64


def level_of(stream_key, extent, shards, smallest, top_value):
    level, own = 1.0, jax.random.fold_in(stream_key, 6)
    for position, parts in shards:
        heights = jnp.exp(jax.random.uniform(jax.random.fold_in(own, position), (parts,), jnp.float32, smallest / len(shards), top_value / len(shards)))
        level = level * jnp.repeat(heights, extent[position] // parts).reshape([-1 if axis == position else 1 for axis in range(len(extent))])
    return level


def shared_out(own_key, own, number, rows, amount, top, most, slope):
    ranking = jax.random.permutation(own_key, amount)
    crowded, common = shares(amount, rows * top, most, slope, True), shares(amount, rows * top, most, slope, False)
    places = jnp.arange(amount)

    def named(tallies, rotation):
        used = int((tallies > 0).sum())
        fixed = max(1, used // 4)
        shifted = fixed + (places - fixed + rotation * (used - fixed)) % max(1, amount - fixed)
        return jnp.zeros((amount,), jnp.int32).at[ranking[jnp.where(places < fixed, places, shifted)]].set(jnp.asarray(tallies, jnp.int32))

    tallies = jnp.where(number % 4 == 0, named(crowded, number // 4), named(common, number - number // 4 - 1))
    mixed = jax.random.permutation(jax.random.fold_in(own, 3), amount)
    source_of, receiver = mixed[0:amount // 2 * 2:2], mixed[1:amount // 2 * 2:2]
    room = jnp.minimum(tallies[source_of] - 1, most - tallies[receiver]) // 2
    room = jnp.where((source_of == ranking[0]) | (receiver == ranking[0]) | (tallies[receiver] == 0), 0, jnp.maximum(room, 0))
    shifted = jax.random.randint(jax.random.fold_in(own, 4), (amount // 2,), 0, 1 << 20) % (room + 1)
    tallies = tallies.at[source_of].add(-shifted).at[receiver].add(shifted)
    labels = jnp.searchsorted(jnp.cumsum(tallies), jnp.arange(rows * top), side="right").astype(jnp.int32)
    listing = labels.reshape(top, rows).T
    listing = listing[jax.random.permutation(jax.random.fold_in(own, 1), rows)]
    rotation = jax.random.randint(jax.random.fold_in(own, 2), (rows, 1), 0, top)
    return jnp.take_along_axis(listing, (jnp.arange(top)[None, :] + rotation) % top, axis=1)


def shares(amount, total, bound, lean, full):
    weights = [(1 << 20) // math.isqrt(standing ** lean) + 1 for standing in range(1, amount + 1)]
    largest = bound if full else min(bound, max(-(-total // amount), total * weights[0] // sum(weights)))
    least = 1 if total - largest >= amount - 1 else 0
    given, rest = [largest] + [least] * (amount - 1), total - largest - least * (amount - 1)
    while rest > 0:
        movable = [i for i in range(1, amount) if given[i] < largest] or [i for i in range(1, amount) if given[i] < bound]
        pool, left = sum([weights[i] for i in movable]), rest
        for i in movable:
            more = min(bound - given[i], max(1, left * weights[i] // pool), rest)
            given[i] = given[i] + more
            rest = rest - more
    return np.array(given)


def normal_values(own_key, extent, width, bound, shards=(), kind=jnp.bfloat16):
    drawn = jax.random.normal(own_key, extent, jnp.float32) * width
    if len(shards) > 0:
        drawn = level_of(own_key, extent, shards, -0.22, 0.18) * drawn
    return jnp.clip(drawn, min=-bound, max=bound).astype(kind)


def setup_inputs(seed: int = 0, part: int = 0) -> dict:
    key_of = jax.random.split(jax.random.key(seed), 8)
    part_splits = jax.random.split(jax.random.fold_in(key_of[7], part), 8)
    tokens = normal_values(part_splits[0], (TOKENS, D), 1.0, 6.0, ((0, 16),))
    norm_gain = jnp.clip(1.0 + 0.15 * jax.random.normal(key_of[1], (LAYERS, D), jnp.float32), 0.25, 1.75).astype(jnp.bfloat16)
    w_gate = normal_values(key_of[2], (LAYERS, D, EXPERTS * FF), D ** -0.5, 0.109375, ((2, 16),))
    w_up = normal_values(key_of[3], (LAYERS, D, EXPERTS * FF), D ** -0.5, 0.109375, ((2, 16),))
    w_down = normal_values(key_of[4], (LAYERS, EXPERTS * FF, D), FF ** -0.5, 0.109375, ((1, 16),))
    routes_keys = jax.random.split(jax.random.fold_in(part_splits[5], 1), LAYERS * TOKENS // TOK_DEV)
    routes_turns = jax.random.permutation(jax.random.fold_in(part_splits[5], 3), LAYERS * TOKENS // TOK_DEV)
    routes = jax.vmap(lambda own, number: shared_out(jax.random.fold_in(part_splits[5], 2), own, number, TOK_DEV, EXPERTS, TOP, CAP, 2))(routes_keys, routes_turns).reshape((LAYERS, TOKENS, TOP))
    gates = jnp.clip(0.1 + 0.9 * jax.random.uniform(part_splits[6], (LAYERS, TOKENS, TOP), jnp.float32) ** level_of(part_splits[6], (LAYERS, TOKENS, TOP), ((1, 16),), -0.2, 0.2), 0.1, 1.0)
    return dict(tokens=tokens, norm_gain=norm_gain, w_gate=w_gate, w_up=w_up, w_down=w_down, routes=routes, gates=gates)


def rms_normed(hidden_state, gain_row):
    widened = hidden_state.astype(jnp.float32)
    scale_inv = lax.rsqrt(lax.optimization_barrier(jnp.mean(widened * widened, axis=-1, keepdims=True)) + 1e-05)
    return (widened * scale_inv * gain_row.astype(jnp.float32)).astype(jnp.bfloat16)

def reference(tokens, norm_gain, w_gate, w_up, w_down, routes, gates):
    block_count = TOKENS // TOK_DEV
    hidden_state = tokens
    for layer_idx in range(LAYERS):
        widened = hidden_state.astype(jnp.float32)
        normed = rms_normed(hidden_state, norm_gain[layer_idx])
        expert_ids = routes[layer_idx].reshape(block_count, TOK_DEV * TOP)
        one_hot = (expert_ids[:, :, None] == jnp.arange(EXPERTS, dtype=jnp.int32)[None, None, :]).astype(jnp.int32)
        slot_index = lax.optimization_barrier(jnp.sum((jnp.cumsum(one_hot, axis=1) - one_hot) * one_hot, axis=2))
        block_ids = jnp.arange(block_count, dtype=jnp.int32)[:, None]
        row_index = (expert_ids * (block_count * CAP) + block_ids * CAP + slot_index).reshape(-1).astype(jnp.int32)
        token_index = jnp.arange(TOKENS * TOP, dtype=jnp.int32) // TOP
        packed = jnp.zeros((EXPERTS * block_count * CAP, D), jnp.bfloat16).at[row_index].set(normed[token_index])
        packed = packed.reshape(EXPERTS, block_count * CAP, D)
        gate_layer = w_gate[layer_idx]
        up_layer = w_up[layer_idx]
        down_layer = w_down[layer_idx]

        def one_expert(expert_num):
            col_start = (expert_num * FF).astype(jnp.int32)
            inputs_f = lax.dynamic_index_in_dim(packed, expert_num, 0, keepdims=False).astype(jnp.float32)
            gate_cols = lax.dynamic_slice_in_dim(gate_layer, col_start, FF, 1).astype(jnp.float32)
            up_cols = lax.dynamic_slice_in_dim(up_layer, col_start, FF, 1).astype(jnp.float32)
            down_rows = lax.dynamic_slice_in_dim(down_layer, col_start, FF, 0).astype(jnp.float32)
            gate_val = jnp.dot(inputs_f, gate_cols)
            up_val = jnp.dot(inputs_f, up_cols)
            active = (gate_val * jax.nn.sigmoid(1.702 * gate_val) * (up_val + 1.0)).astype(jnp.bfloat16)
            active = lax.optimization_barrier(active).astype(jnp.float32)
            return jnp.dot(active, down_rows)
        expert_out = lax.map(one_expert, jnp.arange(EXPERTS, dtype=jnp.int32))
        route_out = expert_out.reshape(-1, D)[row_index].reshape(TOKENS, TOP, D)
        mixture = lax.optimization_barrier(jnp.sum(route_out * gates[layer_idx][:, :, None].astype(jnp.float32), axis=1))
        hidden_state = (widened + mixture).astype(jnp.bfloat16)
    return hidden_state
```

```python
import functools

import jax
import jax.numpy as jnp
from jax import lax
from jax.experimental import pallas as pl
from jax.experimental.pallas import tpu as pltpu
from jax.sharding import PartitionSpec as P

MESH = pl.DeviceIdType.MESH
EPS = 1e-05
TILE = 512
PARTS = 3
MXU = 256


def col_tiles(start, stop, width):
    tiles = []
    while start < stop:
        tiles.append((start, min(width, stop - start)))
        start += width
    return tiles


def tiled_loop(start, stop, width, body):
    full = (stop - start) // width
    if full > 1:
        @pl.loop(0, full)
        def _(i):
            body(pl.multiple_of(start + i * width, 128), width)
    elif full == 1:
        body(start, width)
    if (stop - start) % width:
        body(start + full * width, (stop - start) % width)


def dot_rows(left, right):
    return lax.dot_general(
        left, right, (((1,), (1,)), ((), ())), preferred_element_type=jnp.float32
    )


def tiled(chips, rows, d_model, ff):
    tokens = 2 * chips * rows
    blocks = -(-ff // MXU)
    tails = (d_model % MXU, ff % MXU)
    return (
        tokens % 16 == 0
        and blocks * (tokens // 4) <= 256
        and all(tail and tail % 16 == 0 for tail in tails)
        and tails[0] <= 128
    )


def filled(block, size):
    short = size - block.shape[0]
    if short == 0:
        return block
    return jnp.concatenate([block, jnp.zeros((short, block.shape[1]), block.dtype)], axis=0)


def kernel(
    chips, chips_per_expert, tok_ref, gain_ref, wg_hbm, wu_hbm, wd_hbm, routes_ref, gates_ref,
    out_ref,
    wg, wu, wd, gathered, stacked, x_buf, act, y_buf, peer_buf, blocks, back, hidden,
    w_sem, ag_send, ag_recv, fw_send, fw_recv, pr_send, pr_recv, rs_send, rs_recv,
    *tails, accs=None,
):
    me = lax.axis_index("expert")
    core = lax.axis_index("dp")
    other = 1 - core
    layers, ff, d_model = wd_hbm.shape
    rows = tok_ref.shape[0]
    fast = accs is not None
    whole = d_model // MXU * MXU
    rest = d_model - whole
    strips = -(-ff // MXU)
    half = chips * rows
    step = -(-d_model // (128 * PARTS)) * 128
    parts = col_tiles(0, d_model, step)

    if fast:
        wg_raw, wu_raw, wd_raw, wg_rest, wu_rest, wd_rest = tails
        ups = ((wg_hbm, wg, wg_raw, wg_rest), (wu_hbm, wu, wu_raw, wu_rest))

    def strip_copy(layer, i, f):
        src, dst = ups[i][:2]
        height = pl.ds(f * MXU, min(MXU, ff - f * MXU))
        return pltpu.make_async_copy(
            src.at[layer, height, pl.ds(0, whole)], dst.at[layer, height, :], w_sem.at[layer, i, f]
        )

    def rest_copy(layer, i):
        src, raw = (ups[0][0], wg_raw) if i == 0 else (ups[1][0], wu_raw) if i == 1 else (wd_hbm, wd_raw)
        return pltpu.make_async_copy(
            src.at[layer, :, pl.ds(whole, rest)],
            raw.at[layer, pl.ds(0, ff), :],
            w_sem.at[layer, i, strips],
        )

    def down_copy(layer):
        return pltpu.make_async_copy(
            wd_hbm.at[layer, :, pl.ds(0, whole)], wd.at[layer], w_sem.at[layer, 2, 0]
        )

    def weights(layer):
        if fast:
            return (
                [rest_copy(layer, i) for i in range(2)]
                + [strip_copy(layer, i, f) for f in range(strips) for i in range(2)]
                + [rest_copy(layer, 2), down_copy(layer)]
            )
        pairs = ((wg_hbm, wg), (wu_hbm, wu), (wd_hbm, wd))
        return [
            pltpu.make_async_copy(src.at[layer], dst.at[layer], w_sem.at[layer, i])
            for i, (src, dst) in enumerate(pairs)
        ]

    def turn(layer, i, f):
        _, dst, raw, turned = ups[i]
        strip_copy(layer, i, f).wait()
        if f == 0:
            rest_copy(layer, i).wait()
        height = pl.ds(f * MXU, MXU)
        for k in range(whole // MXU):
            cols = pl.ds(k * MXU, MXU)
            dst[layer, height, cols] = dst[layer, height, cols].T
        turned[layer, :, height] = raw[layer, height, :].T

    def turn_all(layer, pieces):
        for i, f in pieces:
            turn(layer, i, f)

    def pad_down(layer):
        rest_copy(layer, 2).wait()
        wd_rest[layer] = jnp.zeros(wd_rest.shape[1:], wd_rest.dtype)
        wd_rest[layer, pl.ds(0, ff), pl.ds(0, rest)] = wd_raw[layer, pl.ds(0, ff), :]

    def multiply_up(layer, k_range, finish):
        for f in range(strips):
            height = pl.ds(f * MXU, MXU)
            for k in k_range:
                left = x_buf[:, pl.ds(k * MXU, MXU)]
                for i in range(2):
                    _, dst, _, turned = ups[i]
                    if (k + 1) * MXU <= whole:
                        tile = dst[layer, height, pl.ds(k * MXU, MXU)]
                    else:
                        tile = filled(turned[layer, :, height], MXU)
                    register = (f * len(k_range) + k) % 2
                    pltpu.matmul_push_rhs(tile, staging_register=register, mxu_index=i)
                    pltpu.matmul_acc_lhs(accs[i][f], left, load_staged_rhs=register)
            if finish:
                g = pltpu.matmul_pop(accs[0][f])
                u = pltpu.matmul_pop(accs[1][f])
                value = g * jax.nn.sigmoid(1.702 * g) * (u + 1.0)
                if (f + 1) * MXU > ff:
                    place = lax.broadcasted_iota(jnp.int32, value.shape, 1)
                    value = jnp.where(place < ff - f * MXU, value, 0.0)
                act[:, height] = value.astype(jnp.bfloat16)

    def multiply_down(layer, n):
        acc = accs[n % 2][n // 2 % strips]
        cols = pl.ds(n * MXU, MXU)
        for k in range(strips):
            height = pl.ds(k * MXU, min(MXU, ff - k * MXU))
            tile = wd[layer, height, cols] if (n + 1) * MXU <= whole else wd_rest[layer, height, :]
            pltpu.matmul_push_rhs(filled(tile, MXU), staging_register=k % 2, mxu_index=n % 2)
            pltpu.matmul_acc_lhs(acc, act[:, pl.ds(k * MXU, MXU)], load_staged_rhs=k % 2)
        y = pltpu.matmul_pop(acc)
        width = min(MXU, d_model - n * MXU)
        y_buf[layer, :, :, pl.ds(n * MXU, width)] = y.reshape(2, half, MXU)[:, :, :width]

    unrolled = chips <= 16 and chips & (chips - 1) == 0

    def mirror(flip):
        total = 0
        bit = 1
        while bit < chips:
            own = lax.rem(me // bit, 2)
            total = total + bit * (1 - own if flip & bit else own)
            bit *= 2
        return total

    mirrored = [mirror(flip) for flip in range(chips - 1, 0, -1)] if unrolled else []

    def each_peer(body):
        for peer in mirrored:
            body(peer)
        if not unrolled:
            @pl.loop(1, chips)
            def _(d):
                body(lax.rem(me + d, chips))

    def each_chip(body):
        if unrolled:
            for slot in range(chips):
                body(slot)
        else:
            pl.loop(0, chips)(body)

    def gather_copy(layer, peer, slot):
        return pltpu.make_async_remote_copy(
            src_ref=gathered.at[layer, core, slot],
            dst_ref=gathered.at[layer, core, slot],
            send_sem=ag_send.at[layer, peer],
            recv_sem=ag_recv.at[layer, slot],
            device_id={"expert": peer},
            device_id_type=MESH,
        )

    def forward_copy(layer, half_idx, slot):
        return pltpu.make_async_remote_copy(
            src_ref=gathered.at[layer, half_idx, slot],
            dst_ref=gathered.at[layer, half_idx, slot],
            send_sem=fw_send.at[layer, slot],
            recv_sem=fw_recv.at[layer, slot],
            device_id={"dp": other},
            device_id_type=MESH,
        )

    def pair_copy(layer, part):
        c0, cw = parts[part]
        return pltpu.make_async_remote_copy(
            src_ref=y_buf.at[layer, other, :, pl.ds(c0, cw)],
            dst_ref=peer_buf.at[layer, :, pl.ds(c0, cw)],
            send_sem=pr_send.at[layer, part],
            recv_sem=pr_recv.at[layer, part],
            device_id={"dp": other},
            device_id_type=MESH,
        )

    def home_copy(layer, part, peer, slot_src, slot_dst):
        c0, cw = parts[part]
        return pltpu.make_async_remote_copy(
            src_ref=blocks.at[layer, slot_src, :, pl.ds(c0, cw)],
            dst_ref=back.at[layer, slot_dst, :, pl.ds(c0, cw)],
            send_sem=rs_send.at[layer, part, peer],
            recv_sem=rs_recv.at[layer, part, slot_dst],
            device_id={"expert": peer},
            device_id_type=MESH,
        )

    for copy in weights(0):
        copy.start()

    barrier = pltpu.get_barrier_semaphore()
    each_peer(
        lambda peer: pl.semaphore_signal(
            barrier, inc=1, device_id={"expert": peer}, device_id_type=MESH
        )
    )
    pl.semaphore_signal(barrier, inc=1, device_id={"dp": other}, device_id_type=MESH)

    hidden[...] = tok_ref[...].astype(jnp.float32)
    gains = gain_ref[...].astype(jnp.float32)
    for layer in range(layers):
        x = hidden[...]
        scale_inv = lax.rsqrt(jnp.mean(x * x, axis=-1, keepdims=True) + EPS)
        normed = (x * scale_inv * gains[layer : layer + 1]).astype(jnp.bfloat16)
        gathered[layer, core, me] = normed
        if layer == 0:
            pl.semaphore_wait(barrier, chips)
        each_peer(lambda peer: gather_copy(layer, peer, me).start())
        forward_copy(layer, core, me).start()
        if layer == 0:
            for later in range(1, layers):
                for copy in weights(later):
                    copy.start()
            if fast:
                turn_all(0, [(i, f) for f in range(strips) for i in range(2)])
                pad_down(0)

        def pass_on(peer):
            gather_copy(layer, peer, peer).wait_recv()
            forward_copy(layer, core, peer).start()

        each_peer(pass_on)

        each_chip(lambda slot: forward_copy(layer, other, slot).wait_recv())

        per = 8 // rows
        for h in range(2):
            @pl.loop(0, chips // per)
            def _(q):
                stacked[h, q] = jnp.concatenate(
                    [gathered[layer, h, q * per + i].astype(jnp.float32) for i in range(per)], axis=0
                )
        x_buf[:, pl.ds(0, d_model)] = stacked[...].reshape(2 * half, d_model).astype(jnp.bfloat16)
        if fast:
            short = x_buf.shape[1] - d_model
            x_buf[:, pl.ds(d_model, short)] = jnp.zeros((2 * half, short), jnp.bfloat16)
        else:
            w_gate, w_up, w_down = weights(layer)
            w_gate.wait()
            w_up.wait()

        def up_tile(c0, cw):
            cols = pl.ds(c0, cw)
            g = dot_rows(wg[layer, cols, :], x_buf[...]).T
            u = dot_rows(wu[layer, cols, :], x_buf[...]).T
            act[:, cols] = (g * jax.nn.sigmoid(1.702 * g) * (u + 1.0)).astype(jnp.bfloat16)

        if fast:
            multiply_up(layer, range(x_buf.shape[1] // MXU), True)
            down_copy(layer).wait()
        else:
            tiled_loop(0, ff, TILE, up_tile)
            w_down.wait()

        def down_tile(c0, cw):
            cols = pl.ds(c0, cw)
            y = jnp.dot(act[...], wd[layer, :, cols], preferred_element_type=jnp.float32)
            y_buf[layer, :, :, cols] = y.reshape(2, half, cw)

        def send_home(part):
            c0, cw = parts[part]
            cols = pl.ds(c0, cw)
            pair_copy(layer, part).wait_recv()

            @pl.loop(0, chips // per)
            def _(q):
                group = pl.ds(pl.multiple_of(q * 8, 8), 8)
                total = y_buf[layer, core, group, cols] + peer_buf[layer, group, cols]
                for i in range(per):
                    blocks[layer, q * per + i, :, cols] = total[i * rows : (i + 1) * rows].astype(
                        jnp.bfloat16
                    )

            each_peer(lambda peer: home_copy(layer, part, peer, peer, me).start())

        for part, (c0, cw) in enumerate(parts):
            if fast:
                for n in range(c0 // MXU, -(-(c0 + cw) // MXU)):
                    multiply_down(layer, n)
            else:
                tiled_loop(c0, c0 + cw, TILE, down_tile)
            pair_copy(layer, part).start()
            if part > 0:
                send_home(part - 1)
        send_home(len(parts) - 1)
        if fast and layer + 1 < layers:
            turn_all(layer + 1, [(i, f) for f in range(strips) for i in range(2)])
            pad_down(layer + 1)

        routes = routes_ref[layer]
        gates = gates_ref[layer]

        def weight_of(chip):
            expert = chip // chips_per_expert
            return jnp.sum(jnp.where(routes == expert, gates, 0.0), axis=1, keepdims=True)

        hidden[...] += weight_of(me) * blocks[layer, me].astype(jnp.float32)

        def take(peer):
            for part in range(len(parts)):
                home_copy(layer, part, peer, peer, peer).wait_recv()
            hidden[...] += weight_of(peer) * back[layer, peer].astype(jnp.float32)

        each_peer(take)
        result = hidden[...].astype(jnp.bfloat16)
        if layer + 1 < layers:
            hidden[...] = result.astype(jnp.float32)
        else:
            out_ref[...] = result

    for layer in range(layers):
        each_chip(lambda slot: forward_copy(layer, core, slot).wait_send())

        def sent(peer):
            gather_copy(layer, peer, me).wait_send()
            for part in range(len(parts)):
                home_copy(layer, part, peer, peer, me).wait_send()

        each_peer(sent)
        for part in range(len(parts)):
            pair_copy(layer, part).wait_send()


def on_device(tokens, norm_gain, w_gate, w_up, w_down, routes, gates, *, expert_total_of):
    chips = lax.axis_size("expert")
    cores = lax.axis_size("dp")
    rows, d_model = tokens.shape
    layers, _, ff = w_gate.shape
    expert_total = expert_total_of(d_model, ff, chips * cores)
    half = chips * rows
    vmem = pl.BlockSpec(memory_space=pltpu.VMEM)
    hbm = pl.BlockSpec(memory_space=pl.ANY)
    dma = pltpu.SemaphoreType.DMA
    parts = len(col_tiles(0, d_model, -(-d_model // (128 * PARTS)) * 128))
    bf16, f32 = jnp.bfloat16, jnp.float32
    fast = tiled(chips, rows, d_model, ff)
    strips = -(-ff // MXU)
    whole, high = d_model // MXU * MXU, strips * MXU
    rest, wide = d_model - whole, -(-d_model // MXU) * MXU
    body = functools.partial(kernel, chips, chips // expert_total)
    if fast:
        ups = [pltpu.VMEM((layers, high, whole), bf16)] * 2 + [pltpu.VMEM((layers, ff, whole), bf16)]
        tails = [pltpu.VMEM((layers, high, rest), bf16)] * 3
        tails += [pltpu.VMEM((layers, rest, high), bf16)] * 2 + [pltpu.VMEM((layers, high, MXU), bf16)]
        x_shape, act_shape, w_sems = (2 * half, wide), (2 * half, high), (layers, 3, strips + 1)

        def body(*refs):
            each = [pltpu.ACC(i)((2 * half, MXU), f32) for i in range(2) for _ in range(strips)]
            pl.run_scoped(
                lambda *accs: kernel(
                    chips, chips // expert_total, *refs, accs=(accs[:strips], accs[strips:])
                ),
                *each,
            )
    else:
        ups, tails = [pltpu.VMEM((layers, ff, d_model), bf16)] * 3, []
        x_shape, act_shape, w_sems = (2 * half, d_model), (2 * half, ff), (layers, 3)
    return pl.pallas_call(
        body,
        out_shape=jax.ShapeDtypeStruct(tokens.shape, tokens.dtype),
        in_specs=[vmem, vmem, hbm, hbm, hbm, vmem, vmem],
        out_specs=vmem,
        scratch_shapes=[
            *ups,
            pltpu.VMEM((layers, 2, chips, rows, d_model), bf16),
            pltpu.VMEM((2, half // 8, 8, d_model), f32),
            pltpu.VMEM(x_shape, bf16),
            pltpu.VMEM(act_shape, bf16),
            pltpu.VMEM((layers, 2, half, d_model), f32),
            pltpu.VMEM((layers, half, d_model), f32),
            pltpu.VMEM((layers, chips, rows, d_model), bf16),
            pltpu.VMEM((layers, chips, rows, d_model), bf16),
            pltpu.VMEM((rows, d_model), f32),
            dma(w_sems),
            dma((layers, chips)),
            dma((layers, chips)),
            dma((layers, chips)),
            dma((layers, chips)),
            dma((layers, parts)),
            dma((layers, parts)),
            dma((layers, parts, chips)),
            dma((layers, parts, chips)),
            *tails,
        ],
        compiler_params=pltpu.CompilerParams(
            collective_id=0, has_side_effects=True, vmem_limit_bytes=67043328
        ),
    )(
        tokens,
        norm_gain,
        jnp.swapaxes(w_gate, 1, 2),
        jnp.swapaxes(w_up, 1, 2),
        w_down,
        routes,
        gates,
    )


def solution(mesh):
    def expert_total_of(d_model, ff, devices):
        return devices * ff // d_model

    return jax.shard_map(
        functools.partial(on_device, expert_total_of=expert_total_of),
        mesh=mesh,
        in_specs=(
            P(("groups", "expert", "dp"), None),
            P(),
            P(None, None, ("expert", "dp")),
            P(None, None, ("expert", "dp")),
            P(None, ("expert", "dp"), None),
            P(None, ("groups", "expert", "dp"), None),
            P(None, ("groups", "expert", "dp"), None),
        ),
        out_specs=P(("groups", "expert", "dp"), None),
        check_vma=False,
    )
```

```python
import functools

import jax
import jax.numpy as jnp
from jax import lax
from jax.experimental import pallas as pl
from jax.experimental.pallas import tpu as pltpu
from jax.sharding import PartitionSpec as P

MESH = pl.DeviceIdType.MESH
EPS = 1e-05
TILE = 512
PARTS = 2
CUTS = 1
CAP = 3
MXU = 256


def col_tiles(start, stop, width):
    tiles = []
    while start < stop:
        tiles.append((start, min(width, stop - start)))
        start += width
    return tiles


def tiled_loop(start, stop, width, body):
    full = (stop - start) // width
    if full > 1:
        @pl.loop(0, full)
        def _(i):
            body(pl.multiple_of(start + i * width, 128), width)
    elif full == 1:
        body(start, width)
    if (stop - start) % width:
        body(start + full * width, (stop - start) % width)


def dot_rows(left, right):
    return lax.dot_general(
        left, right, (((1,), (1,)), ((), ())), preferred_element_type=jnp.float32
    )


def folded(d_model):
    for main in range(MXU, d_model, MXU):
        pad = -(-(d_model - main) // 128) * 128
        if CAP * pad <= main and (CAP - 1) * pad % MXU == 0:
            return main, pad
    return None


def tiled(chips, chips_per_expert, rows, d_model, ff):
    tokens = 2 * chips * rows
    blocks = -(-ff // MXU)
    tails = (d_model % MXU, ff % MXU)
    return (
        chips <= 16
        and chips & (chips - 1) == 0
        and chips_per_expert == 1
        and rows == CAP + 1
        and folded(d_model) is not None
        and tokens % 16 == 0
        and blocks * (tokens // 4) <= 256
        and all(tail and tail % 16 == 0 for tail in tails)
        and tails[0] <= 128
    )


def filled(block, size):
    short = size - block.shape[0]
    if short == 0:
        return block
    return jnp.concatenate([block, jnp.zeros((short, block.shape[1]), block.dtype)], axis=0)


def kernel(
    chips, chips_per_expert, tok_hbm, gain_hbm, wg_hbm, wu_hbm, wd_hbm, routes_hbm, gates_hbm,
    out_ref,
    wg, wu, wd, gathered, stacked, x_buf, act, y_buf, y_half, peer_buf, blocks, back, hidden,
    w_sem, ag_send, ag_recv, fw_send, fw_recv, pr_send, pr_recv, rs_send, rs_recv,
    tok_ref, gain_ref, routes_ref, gates_ref, in_sem, *tails, accs=None,
):
    me = lax.axis_index("expert")
    core = lax.axis_index("dp")
    other = 1 - core
    layers, ff, d_model = wd_hbm.shape
    rows = tok_ref.shape[0]
    fast = accs is not None
    whole = d_model // MXU * MXU
    rest = d_model - whole
    strips = -(-ff // MXU)
    half = chips * rows
    step = -(-d_model // (128 * PARTS)) * 128
    parts = col_tiles(0, d_model, step)
    cuts = col_tiles(0, d_model, -(-d_model // (MXU * CUTS)) * MXU)
    if fast:
        main, pad = folded(d_model)
        cuts = [(0, main)]
        parts = [(0, (CAP - 1) * pad), ((CAP - 1) * pad, main - (CAP - 1) * pad)]
        pair_lanes = [(0, pad + parts[0][1]), (pad + parts[0][1], parts[1][1])]
    else:
        pair_lanes = parts

    if fast:
        wg_raw, wu_raw, wd_raw, wg_rest, wu_rest, wd_rest, packed, norm_buf, route_nums, slots = tails
        ups = ((wg_hbm, wg, wg_raw, wg_rest), (wu_hbm, wu, wu_raw, wu_rest))

    def strip_copy(layer, i, f):
        src, dst = ups[i][:2]
        height = pl.ds(f * MXU, min(MXU, ff - f * MXU))
        return pltpu.make_async_copy(
            src.at[layer, height, pl.ds(0, whole)], dst.at[layer, height, :], w_sem.at[layer, i, f]
        )

    def rest_copy(layer, i):
        src, raw = (ups[0][0], wg_raw) if i == 0 else (ups[1][0], wu_raw) if i == 1 else (wd_hbm, wd_raw)
        return pltpu.make_async_copy(
            src.at[layer, :, pl.ds(whole, rest)],
            raw.at[layer, pl.ds(0, ff), :],
            w_sem.at[layer, i, strips],
        )

    def down_copy(layer):
        return pltpu.make_async_copy(
            wd_hbm.at[layer, :, pl.ds(0, whole)], wd.at[layer], w_sem.at[layer, 2, 0]
        )

    def weights(layer):
        if fast:
            return (
                [rest_copy(layer, i) for i in range(2)]
                + [strip_copy(layer, i, f) for f in range(strips) for i in range(2)]
                + [rest_copy(layer, 2), down_copy(layer)]
            )
        pairs = ((wg_hbm, wg), (wu_hbm, wu), (wd_hbm, wd))
        return [
            pltpu.make_async_copy(src.at[layer], dst.at[layer], w_sem.at[layer, i])
            for i, (src, dst) in enumerate(pairs)
        ]

    def turn(layer, i, f):
        _, dst, raw, turned = ups[i]
        strip_copy(layer, i, f).wait()
        if f == 0:
            rest_copy(layer, i).wait()
        height = pl.ds(f * MXU, MXU)
        for k in range(whole // MXU):
            cols = pl.ds(k * MXU, MXU)
            dst[layer, height, cols] = dst[layer, height, cols].T
        turned[layer, :, height] = raw[layer, height, :].T

    def turn_all(layer, pieces):
        for i, f in pieces:
            turn(layer, i, f)

    def pad_down(layer):
        rest_copy(layer, 2).wait()
        wd_rest[layer] = jnp.zeros(wd_rest.shape[1:], wd_rest.dtype)
        wd_rest[layer, pl.ds(0, ff), pl.ds(0, rest)] = wd_raw[layer, pl.ds(0, ff), :]

    def multiply_up(layer, k_range, finish):
        for f in range(strips):
            height = pl.ds(f * MXU, MXU)
            for k in k_range:
                left = x_buf[:, pl.ds(k * MXU, MXU)]
                for i in range(2):
                    _, dst, _, turned = ups[i]
                    if (k + 1) * MXU <= whole:
                        tile = dst[layer, height, pl.ds(k * MXU, MXU)]
                    else:
                        tile = filled(turned[layer, :, height], MXU)
                    register = (f * len(k_range) + k - k_range[0]) % 2
                    pltpu.matmul_push_rhs(tile, staging_register=register, mxu_index=i)
                    pltpu.matmul_acc_lhs(accs[i][f], left, load_staged_rhs=register)
            if finish:
                g = pltpu.matmul_pop(accs[0][f])
                u = pltpu.matmul_pop(accs[1][f])
                value = g * jax.nn.sigmoid(1.702 * g) * (u + 1.0)
                if (f + 1) * MXU > ff:
                    place = lax.broadcasted_iota(jnp.int32, value.shape, 1)
                    value = jnp.where(place < ff - f * MXU, value, 0.0)
                act[:, height] = value.astype(jnp.bfloat16)

    def multiply_down(layer, n):
        acc = accs[n % 2][n // 2 % strips]
        cols = pl.ds(n * MXU, MXU)
        for k in range(strips):
            height = pl.ds(k * MXU, min(MXU, ff - k * MXU))
            tile = wd[layer, height, cols] if (n + 1) * MXU <= whole else wd_rest[layer, height, :]
            pltpu.matmul_push_rhs(filled(tile, MXU), staging_register=k % 2, mxu_index=n % 2)
            pltpu.matmul_acc_lhs(acc, act[:, pl.ds(k * MXU, MXU)], load_staged_rhs=k % 2)
        y = pltpu.matmul_pop(acc)
        width = min(MXU, main + pad - n * MXU)
        lane = n * MXU - main if n * MXU >= main else pad + n * MXU
        y = y.reshape(2, half, MXU)[:, :, :width]
        y_buf[layer, :, :, pl.ds(lane, width)] = y
        y_half[layer, :, :, pl.ds(lane, width)] = y.astype(jnp.bfloat16)

    def number_slots(layer):
        for chip in range(chips):
            count = jnp.int32(0)
            for t in range(rows):
                named = route_nums[layer, t, 0] == chip
                for k in range(1, route_nums.shape[2]):
                    named = named | (route_nums[layer, t, k] == chip)
                slots[layer, chip, t] = jnp.where(named, count, -1)
                count = count + jnp.where(named, 1, 0)

    def pack(layer, chip):
        spots = [slots[layer, chip, t] for t in range(rows)]

        def piece(lane, width, j):
            place = lax.broadcasted_iota(jnp.int32, (rows, width), 0)
            value = jnp.zeros((rows, width), jnp.float32)
            for t in range(rows):
                row = jnp.broadcast_to(norm_buf[t : t + 1, pl.ds(lane, width)], (rows, width))
                value = jnp.where(place == spots[t], row, value)
            if j is not None:
                for t in range(rows):
                    row = jnp.broadcast_to(norm_buf[t : t + 1, pl.ds(main, width)], (rows, width))
                    spot = jnp.where(spots[t] == j, CAP, -1)
                    value = jnp.where(place == spot, row, value)
            return value.astype(jnp.bfloat16)

        pieces = [piece(j * pad, pad, j) for j in range(CAP)]
        if CAP * pad < main:
            pieces.append(piece(CAP * pad, main - CAP * pad, None))
        return jnp.concatenate(pieces, axis=1)

    def unfold(value):
        place = lax.rem(lax.broadcasted_iota(jnp.int32, (8, pad), 0), rows)
        total = jnp.zeros((8, pad), jnp.float32)
        for j in range(CAP):
            moved = pltpu.roll(value[:, j * pad : (j + 1) * pad], 8 + j - CAP, 0)
            total = jnp.where(place == j, moved, total)
        return total

    def fold(part, middle, end):
        c0, cw = parts[part]
        place = lax.rem(lax.broadcasted_iota(jnp.int32, (8, pad), 0), rows)
        pieces = []
        lane = 0
        for j in range(CAP):
            if c0 <= j * pad < c0 + cw:
                moved = pltpu.roll(end, CAP - j, 0)
                pieces.append(jnp.where(place == CAP, moved, middle[:, lane : lane + pad]))
                lane += pad
        if lane < cw:
            pieces.append(middle[:, lane:])
        return jnp.concatenate(pieces, axis=1) if len(pieces) > 1 else pieces[0]

    unrolled = chips <= 16 and chips & (chips - 1) == 0

    def mirror(flip):
        total = 0
        bit = 1
        while bit < chips:
            own = lax.rem(me // bit, 2)
            total = total + bit * (1 - own if flip & bit else own)
            bit *= 2
        return total

    mirrored = [mirror(flip) for flip in range(chips - 1, 0, -1)] if unrolled else []

    def each_peer(body):
        for peer in mirrored:
            body(peer)
        if not unrolled:
            @pl.loop(1, chips)
            def _(d):
                body(lax.rem(me + d, chips))

    def near_peers(body):
        for peer in mirrored[::-1]:
            body(peer)
        if not unrolled:
            each_peer(body)

    def each_group(count, body):
        if fast:
            for q in range(count):
                body(q)
        else:
            pl.loop(0, count)(body)

    def each_chip(body):
        if unrolled:
            for slot in range(chips):
                body(slot)
        else:
            pl.loop(0, chips)(body)

    def gather_copy(layer, cut, half_idx, peer, slot):
        block = gathered.at[layer, half_idx, slot, :, pl.ds(*cuts[cut])]
        return pltpu.make_async_remote_copy(
            src_ref=packed.at[layer, peer] if fast else block,
            dst_ref=block,
            send_sem=ag_send.at[layer, cut, peer],
            recv_sem=ag_recv.at[layer, cut, slot],
            device_id={"expert": peer, "dp": other},
            device_id_type=MESH,
        )

    def forward_copy(layer, cut, half_idx, slot):
        block = gathered.at[layer, half_idx, slot, :, pl.ds(*cuts[cut])]
        return pltpu.make_async_remote_copy(
            src_ref=block,
            dst_ref=block,
            send_sem=fw_send.at[layer, cut, slot],
            recv_sem=fw_recv.at[layer, cut, slot],
            device_id={"dp": other},
            device_id_type=MESH,
        )

    def pair_copy(layer, part):
        c0, cw = pair_lanes[part]
        return pltpu.make_async_remote_copy(
            src_ref=y_half.at[layer, core, :, pl.ds(c0, cw)],
            dst_ref=peer_buf.at[layer, :, pl.ds(c0, cw)],
            send_sem=pr_send.at[layer, part],
            recv_sem=pr_recv.at[layer, part],
            device_id={"dp": other},
            device_id_type=MESH,
        )

    def home_copy(layer, part, peer, slot_src, slot_dst):
        c0, cw = parts[part]
        return pltpu.make_async_remote_copy(
            src_ref=blocks.at[layer, slot_src, :, pl.ds(c0, cw)],
            dst_ref=back.at[layer, slot_dst, :, pl.ds(c0, cw)],
            send_sem=rs_send.at[layer, part, peer],
            recv_sem=rs_recv.at[layer, part, slot_dst],
            device_id={"expert": peer, "dp": other},
            device_id_type=MESH,
        )

    def beside_copy(layer, part):
        c0, cw = parts[part]
        return pltpu.make_async_remote_copy(
            src_ref=blocks.at[layer, me, :, pl.ds(c0, cw)],
            dst_ref=back.at[layer, me, :, pl.ds(c0, cw)],
            send_sem=rs_send.at[layer, part, me],
            recv_sem=rs_recv.at[layer, part, me],
            device_id={"dp": other},
            device_id_type=MESH,
        )

    inputs = [
        pltpu.make_async_copy(src, dst, in_sem.at[i])
        for i, (src, dst) in enumerate(
            ((tok_hbm, tok_ref), (gain_hbm, gain_ref), (routes_hbm, routes_ref), (gates_hbm, gates_ref))
        )
    ]
    if fast:
        inputs.append(pltpu.make_async_copy(routes_hbm, route_nums, in_sem.at[4]))
    for copy in inputs:
        copy.start()
    barrier = pltpu.get_barrier_semaphore()
    each_peer(
        lambda peer: pl.semaphore_signal(
            barrier, inc=1, device_id={"expert": peer, "dp": other}, device_id_type=MESH
        )
    )
    pl.semaphore_signal(barrier, inc=1, device_id={"dp": other}, device_id_type=MESH)
    for copy in inputs:
        copy.wait()
    for copy in weights(0):
        copy.start()

    if fast:
        for layer in range(layers):
            number_slots(layer)
        norm_buf[...] = jnp.zeros_like(norm_buf)
    hidden[...] = tok_ref[...].astype(jnp.float32)
    gains = gain_ref[...].astype(jnp.float32)
    for layer in range(layers):
        x = hidden[...]
        scale_inv = lax.rsqrt(jnp.mean(x * x, axis=-1, keepdims=True) + EPS)
        normed = (x * scale_inv * gains[layer : layer + 1]).astype(jnp.bfloat16)
        if fast:
            norm_buf[:, pl.ds(0, d_model)] = normed.astype(jnp.float32)
        else:
            gathered[layer, core, me] = normed
        if layer == 0:
            if fast:
                for peer in mirrored:
                    packed[layer, peer] = pack(layer, peer)
                gathered[layer, core, me] = pack(layer, me)
            pl.semaphore_wait(barrier, chips)
        for cut in range(len(cuts)):
            def hand_out(peer):
                if fast and layer > 0:
                    packed[layer, peer] = pack(layer, peer)
                gather_copy(layer, cut, core, peer, me).start()

            each_peer(hand_out)
            if fast and layer > 0:
                gathered[layer, core, me] = pack(layer, me)
            forward_copy(layer, cut, core, me).start()
        if layer == 0:
            for later in range(1, layers):
                for copy in weights(later):
                    copy.start()
        if fast:
            turn_all(layer, [(i, f) for f in range(strips) for i in range(2) if layer == 0 or i == 1])
            pad_down(layer)

        for cut in range(len(cuts)):
            def pass_on(peer):
                gather_copy(layer, cut, other, peer, peer).wait_recv()
                forward_copy(layer, cut, other, peer).start()

            near_peers(pass_on)

        per = 8 // rows

        def stack(cut):
            c0, cw = cuts[cut]
            cols = pl.ds(c0, cw)
            def lift(h):
                def one_group(q):
                    value = jnp.concatenate(
                        [
                            gathered[layer, h, q * per + i, :, cols].astype(jnp.float32)
                            for i in range(per)
                        ],
                        axis=0,
                    )
                    stacked[h, q, :, cols] = value
                    if fast:
                        stacked[h, q, :, pl.ds(main, pad)] = unfold(value)

                each_group(chips // per, one_group)
                if fast:
                    height = pl.ds(pl.multiple_of(h * half, half), half)
                    lanes = pl.ds(0, main + pad)
                    x_buf[height, lanes] = (
                        stacked[h].reshape(half, main + pad).astype(jnp.bfloat16)
                    )

            forward_copy(layer, cut, other, me).wait_recv()
            if fast:
                lift(other)
            each_peer(lambda peer: forward_copy(layer, cut, core, peer).wait_recv())
            if fast:
                lift(core)
            else:
                lift(0)
                lift(1)
                x_buf[:, cols] = stacked[:, :, :, cols].reshape(2 * half, cw).astype(jnp.bfloat16)

        if fast:
            short = x_buf.shape[1] - main - pad
            if short and layer == 0:
                x_buf[:, pl.ds(main + pad, short)] = jnp.zeros((2 * half, short), jnp.bfloat16)
        else:
            for cut in range(len(cuts)):
                stack(cut)
            w_gate, w_up, w_down = weights(layer)
            w_gate.wait()
            w_up.wait()

        def up_tile(c0, cw):
            cols = pl.ds(c0, cw)
            g = dot_rows(wg[layer, cols, :], x_buf[...]).T
            u = dot_rows(wu[layer, cols, :], x_buf[...]).T
            act[:, cols] = (g * jax.nn.sigmoid(1.702 * g) * (u + 1.0)).astype(jnp.bfloat16)

        if fast:
            for cut, (c0, cw) in enumerate(cuts):
                stack(cut)
                multiply_up(layer, range(-(-d_model // MXU)), True)
            down_copy(layer).wait()
        else:
            tiled_loop(0, ff, TILE, up_tile)
            w_down.wait()

        def down_tile(c0, cw):
            cols = pl.ds(c0, cw)
            y = jnp.dot(act[...], wd[layer, :, cols], preferred_element_type=jnp.float32)
            y_buf[layer, :, :, cols] = y.reshape(2, half, cw)
            y_half[layer, :, :, cols] = y.reshape(2, half, cw).astype(jnp.bfloat16)

        def send_home(part):
            c0, cw = parts[part]
            cols = pl.ds(c0, cw)
            pair_copy(layer, part).wait_recv()

            def one_group(q):
                group = pl.ds(q * 8 if fast else pl.multiple_of(q * 8, 8), 8)
                def added(lanes):
                    mine, theirs = y_buf[layer, other, group, lanes], peer_buf[layer, group, lanes]
                    return mine + theirs.astype(jnp.float32)

                if fast:
                    total = fold(part, added(pl.ds(pad + c0, cw)), added(pl.ds(0, pad)))
                else:
                    total = added(cols)
                for i in range(per):
                    blocks[layer, q * per + i, :, cols] = total[i * rows : (i + 1) * rows].astype(
                        jnp.bfloat16
                    )

            each_group(chips // per, one_group)
            each_peer(lambda peer: home_copy(layer, part, peer, peer, me).start())
            beside_copy(layer, part).start()

        for part, (c0, cw) in enumerate(parts):
            if fast:
                first = range(main // MXU, -(-d_model // MXU)) if part == 0 else ()
                for n in (*first, *range(c0 // MXU, (c0 + cw) // MXU)):
                    multiply_down(layer, n)
            else:
                tiled_loop(c0, c0 + cw, TILE, down_tile)
            pair_copy(layer, part).start()
            if part > 0 and not fast:
                send_home(part - 1)
        for part in range(len(parts)) if fast else [len(parts) - 1]:
            send_home(part)
        if fast and layer + 1 < layers:
            turn_all(layer + 1, [(0, f) for f in range(strips)])

        routes = routes_ref[layer]
        gates = gates_ref[layer]

        def weight_of(chip):
            expert = chip // chips_per_expert
            return jnp.sum(jnp.where(routes == expert, gates, 0.0), axis=1, keepdims=True)

        def shares_of(chip):
            place = lax.broadcasted_iota(jnp.int32, (rows, 1), 0)
            spot = jnp.full((rows, 1), -1, jnp.int32)
            for t in range(rows):
                spot = jnp.where(place == t, slots[layer, chip, t], spot)
            weight = weight_of(chip)
            return [jnp.where(spot == j, weight, 0.0) for j in range(CAP)]

        def add(chip, shares):
            if not fast:
                hidden[...] += weight_of(chip) * back[layer, chip].astype(jnp.float32)
                return
            block = back[layer, chip].astype(jnp.float32)
            middle = sum(shares[j] * block[j : j + 1] for j in range(CAP))
            end = sum(shares[j] * block[CAP : CAP + 1, j * pad : (j + 1) * pad] for j in range(CAP))
            hidden[:, pl.ds(0, main)] += middle
            hidden[:, pl.ds(main, d_model - main)] += end[:, : d_model - main]

        def take(peer, shares=None):
            for part in range(len(parts)):
                home_copy(layer, part, peer, peer, peer).wait_recv()
            add(peer, shares)

        own = shares_of(me) if fast else None
        known = [shares_of(peer) for peer in mirrored[::-1]] if fast else []
        for part in range(len(parts)):
            beside_copy(layer, part).wait_recv()
        add(me, own)
        if fast:
            for peer, shares in zip(mirrored[::-1], known):
                take(peer, shares)
        else:
            near_peers(take)
        result = hidden[...].astype(jnp.bfloat16)
        if layer + 1 < layers:
            hidden[...] = result.astype(jnp.float32)
        else:
            out_ref[...] = result

    for layer in range(layers):
        for cut in range(len(cuts)):
            each_peer(lambda peer: forward_copy(layer, cut, other, peer).wait_send())
            forward_copy(layer, cut, core, me).wait_send()

        def sent(peer):
            for cut in range(len(cuts)):
                gather_copy(layer, cut, core, peer, me).wait_send()
            for part in range(len(parts)):
                home_copy(layer, part, peer, peer, me).wait_send()

        each_peer(sent)
        for part in range(len(parts)):
            pair_copy(layer, part).wait_send()
            beside_copy(layer, part).wait_send()


def on_device(tokens, norm_gain, w_gate, w_up, w_down, routes, gates, *, expert_total_of):
    chips = lax.axis_size("expert")
    cores = lax.axis_size("dp")
    rows, d_model = tokens.shape
    layers, _, ff = w_gate.shape
    expert_total = expert_total_of(d_model, ff, chips * cores)
    half = chips * rows
    vmem = pl.BlockSpec(memory_space=pltpu.VMEM)
    top = routes.shape[-1]
    hbm = pl.BlockSpec(memory_space=pl.ANY)
    dma = pltpu.SemaphoreType.DMA
    parts = len(col_tiles(0, d_model, -(-d_model // (128 * PARTS)) * 128))
    bf16, f32 = jnp.bfloat16, jnp.float32
    fast = tiled(chips, chips // expert_total, rows, d_model, ff)
    main, pad = folded(d_model) if fast else (d_model, 0)
    lanes = main + pad
    strips = -(-ff // MXU)
    whole, high = d_model // MXU * MXU, strips * MXU
    rest, wide = d_model - whole, -(-d_model // MXU) * MXU
    body = functools.partial(kernel, chips, chips // expert_total)
    if fast:
        ups = [pltpu.VMEM((layers, high, whole), bf16)] * 2 + [pltpu.VMEM((layers, ff, whole), bf16)]
        tails = [pltpu.VMEM((layers, high, rest), bf16)] * 3
        tails += [pltpu.VMEM((layers, rest, high), bf16)] * 2 + [pltpu.VMEM((layers, high, MXU), bf16)]
        tails += [
            pltpu.VMEM((layers, chips, rows, main), bf16),
            pltpu.VMEM((rows, lanes), f32),
            pltpu.SMEM((layers, rows, top), jnp.int32),
            pltpu.SMEM((layers, chips, rows), jnp.int32),
        ]
        x_shape, act_shape, w_sems = (2 * half, wide), (2 * half, high), (layers, 3, strips + 1)

        def body(*refs):
            each = [pltpu.ACC(i)((2 * half, MXU), f32) for i in range(2) for _ in range(strips)]
            pl.run_scoped(
                lambda *accs: kernel(
                    chips, chips // expert_total, *refs, accs=(accs[:strips], accs[strips:])
                ),
                *each,
            )
    else:
        ups, tails = [pltpu.VMEM((layers, ff, d_model), bf16)] * 3, []
        x_shape, act_shape, w_sems = (2 * half, d_model), (2 * half, ff), (layers, 3)
    return pl.pallas_call(
        body,
        out_shape=jax.ShapeDtypeStruct(tokens.shape, tokens.dtype),
        in_specs=[hbm] * 7,
        out_specs=vmem,
        scratch_shapes=[
            *ups,
            pltpu.VMEM((layers, 2, chips, rows, main), bf16),
            pltpu.VMEM((2, half // 8, 8, lanes), f32),
            pltpu.VMEM(x_shape, bf16),
            pltpu.VMEM(act_shape, bf16),
            pltpu.VMEM((layers, 2, half, lanes), f32),
            pltpu.VMEM((layers, 2, half, lanes), bf16),
            pltpu.VMEM((layers, half, lanes), bf16),
            pltpu.VMEM((layers, chips, rows, main), bf16),
            pltpu.VMEM((layers, chips, rows, main), bf16),
            pltpu.VMEM((rows, d_model), f32),
            dma(w_sems),
            dma((layers, CUTS, chips)),
            dma((layers, CUTS, chips)),
            dma((layers, CUTS, chips)),
            dma((layers, CUTS, chips)),
            dma((layers, parts)),
            dma((layers, parts)),
            dma((layers, parts, chips)),
            dma((layers, parts, chips)),
            pltpu.VMEM((rows, d_model), bf16),
            pltpu.VMEM((layers, d_model), bf16),
            pltpu.VMEM((layers, rows, top), jnp.int32),
            pltpu.VMEM((layers, rows, top), f32),
            dma((5,)),
            *tails,
        ],
        compiler_params=pltpu.CompilerParams(
            collective_id=0, has_side_effects=True, vmem_limit_bytes=67043328
        ),
    )(
        tokens,
        norm_gain,
        jnp.swapaxes(w_gate, 1, 2),
        jnp.swapaxes(w_up, 1, 2),
        w_down,
        routes,
        gates,
    )


def solution(mesh):
    def expert_total_of(d_model, ff, devices):
        return devices * ff // d_model

    return jax.shard_map(
        functools.partial(on_device, expert_total_of=expert_total_of),
        mesh=mesh,
        in_specs=(
            P(("groups", "expert", "dp"), None),
            P(),
            P(None, None, ("expert", "dp")),
            P(None, None, ("expert", "dp")),
            P(None, ("expert", "dp"), None),
            P(None, ("groups", "expert", "dp"), None),
            P(None, ("groups", "expert", "dp"), None),
        ),
        out_specs=P(("groups", "expert", "dp"), None),
        check_vma=False,
    )
```

```python
import functools

import jax
import jax.numpy as jnp
from jax import lax
from jax.experimental import pallas as pl
from jax.experimental.pallas import tpu as pltpu
from jax.sharding import PartitionSpec as P

MESH = pl.DeviceIdType.MESH
EPS = 1e-05
TILE = 512
PARTS = 2
CUTS = 1
CAP = 3
MXU = 256


def col_tiles(start, stop, width):
    tiles = []
    while start < stop:
        tiles.append((start, min(width, stop - start)))
        start += width
    return tiles


def tiled_loop(start, stop, width, body):
    full = (stop - start) // width
    if full > 1:
        @pl.loop(0, full)
        def _(i):
            body(pl.multiple_of(start + i * width, 128), width)
    elif full == 1:
        body(start, width)
    if (stop - start) % width:
        body(start + full * width, (stop - start) % width)


def dot_rows(left, right):
    return lax.dot_general(
        left, right, (((1,), (1,)), ((), ())), preferred_element_type=jnp.float32
    )


def folded(d_model):
    for main in range(MXU, d_model, MXU):
        pad = -(-(d_model - main) // 128) * 128
        if CAP * pad <= main and (CAP - 1) * pad % MXU == 0:
            return main, pad
    return None


def tiled(chips, chips_per_expert, rows, d_model, ff):
    tokens = 2 * chips * rows
    blocks = -(-ff // MXU)
    tails = (d_model % MXU, ff % MXU)
    return (
        chips <= 16
        and chips & (chips - 1) == 0
        and chips_per_expert == 1
        and rows == CAP + 1
        and folded(d_model) is not None
        and tokens % 16 == 0
        and blocks * (tokens // 4) <= 256
        and all(tail and tail % 16 == 0 for tail in tails)
        and tails[0] <= 128
    )


def filled(block, size):
    short = size - block.shape[0]
    if short == 0:
        return block
    return jnp.concatenate([block, jnp.zeros((short, block.shape[1]), block.dtype)], axis=0)


def kernel(
    chips, chips_per_expert, tok_hbm, gain_hbm, wg_hbm, wu_hbm, wd_hbm, routes_hbm, gates_hbm,
    out_ref,
    wg, wu, wd, gathered, stacked, x_buf, act, y_buf, y_half, peer_buf, blocks, back, hidden,
    w_sem, ag_send, ag_recv, fw_send, fw_recv, pr_send, pr_recv, rs_send, rs_recv,
    tok_ref, gain_ref, routes_ref, gates_ref, in_sem, *tails, accs=None,
):
    me = lax.axis_index("expert")
    core = lax.axis_index("dp")
    other = 1 - core
    layers, ff, d_model = wd_hbm.shape
    rows = tok_ref.shape[0]
    fast = accs is not None
    whole = d_model // MXU * MXU
    rest = d_model - whole
    strips = -(-ff // MXU)
    half = chips * rows
    step = -(-d_model // (128 * PARTS)) * 128
    parts = col_tiles(0, d_model, step)
    cuts = col_tiles(0, d_model, -(-d_model // (MXU * CUTS)) * MXU)
    if fast:
        main, pad = folded(d_model)
        cuts = [(0, main)]
        parts = [(0, (CAP - 1) * pad), ((CAP - 1) * pad, main - (CAP - 1) * pad)]
        pair_lanes = [(0, pad + parts[0][1]), (pad + parts[0][1], parts[1][1])]
    else:
        pair_lanes = parts

    if fast:
        wg_raw, wu_raw, wd_raw, wg_rest, wu_rest, wd_rest, packed, norm_buf, route_nums, slots = tails
        ups = ((wg_hbm, wg, wg_raw, wg_rest), (wu_hbm, wu, wu_raw, wu_rest))

    def strip_copy(layer, i, f):
        src, dst = ups[i][:2]
        height = pl.ds(f * MXU, min(MXU, ff - f * MXU))
        return pltpu.make_async_copy(
            src.at[layer, height, pl.ds(0, whole)], dst.at[layer, height, :], w_sem.at[layer, i, f]
        )

    def rest_copy(layer, i):
        src, raw = (ups[0][0], wg_raw) if i == 0 else (ups[1][0], wu_raw) if i == 1 else (wd_hbm, wd_raw)
        return pltpu.make_async_copy(
            src.at[layer, :, pl.ds(whole, rest)],
            raw.at[layer, pl.ds(0, ff), :],
            w_sem.at[layer, i, strips],
        )

    def down_copy(layer):
        return pltpu.make_async_copy(
            wd_hbm.at[layer, :, pl.ds(0, whole)], wd.at[layer], w_sem.at[layer, 2, 0]
        )

    def weights(layer):
        if fast:
            return (
                [rest_copy(layer, i) for i in range(2)]
                + [strip_copy(layer, i, f) for f in range(strips) for i in range(2)]
                + [rest_copy(layer, 2), down_copy(layer)]
            )
        pairs = ((wg_hbm, wg), (wu_hbm, wu), (wd_hbm, wd))
        return [
            pltpu.make_async_copy(src.at[layer], dst.at[layer], w_sem.at[layer, i])
            for i, (src, dst) in enumerate(pairs)
        ]

    def turn(layer, i, f):
        _, dst, raw, turned = ups[i]
        strip_copy(layer, i, f).wait()
        if f == 0:
            rest_copy(layer, i).wait()
        height = pl.ds(f * MXU, MXU)
        for k in range(whole // MXU):
            cols = pl.ds(k * MXU, MXU)
            dst[layer, height, cols] = dst[layer, height, cols].T
        turned[layer, :, height] = raw[layer, height, :].T

    def turn_all(layer, pieces):
        for i, f in pieces:
            turn(layer, i, f)

    def pad_down(layer):
        rest_copy(layer, 2).wait()
        wd_rest[layer] = jnp.zeros(wd_rest.shape[1:], wd_rest.dtype)
        wd_rest[layer, pl.ds(0, ff), pl.ds(0, rest)] = wd_raw[layer, pl.ds(0, ff), :]

    def multiply_up(layer, k_range, finish):
        for f in range(strips):
            height = pl.ds(f * MXU, MXU)
            for k in k_range:
                left = x_buf[:, pl.ds(k * MXU, MXU)]
                for i in range(2):
                    _, dst, _, turned = ups[i]
                    if (k + 1) * MXU <= whole:
                        tile = dst[layer, height, pl.ds(k * MXU, MXU)]
                    else:
                        tile = filled(turned[layer, :, height], MXU)
                    register = (f * len(k_range) + k - k_range[0]) % 2
                    pltpu.matmul_push_rhs(tile, staging_register=register, mxu_index=i)
                    pltpu.matmul_acc_lhs(accs[i][f], left, load_staged_rhs=register)
            if finish:
                g = pltpu.matmul_pop(accs[0][f])
                u = pltpu.matmul_pop(accs[1][f])
                value = g * jax.nn.sigmoid(1.702 * g) * (u + 1.0)
                if (f + 1) * MXU > ff:
                    place = lax.broadcasted_iota(jnp.int32, value.shape, 1)
                    value = jnp.where(place < ff - f * MXU, value, 0.0)
                act[:, height] = value.astype(jnp.bfloat16)

    def multiply_down(layer, n):
        acc = accs[n % 2][n // 2 % strips]
        cols = pl.ds(n * MXU, MXU)
        for k in range(strips):
            height = pl.ds(k * MXU, min(MXU, ff - k * MXU))
            tile = wd[layer, height, cols] if (n + 1) * MXU <= whole else wd_rest[layer, height, :]
            pltpu.matmul_push_rhs(filled(tile, MXU), staging_register=k % 2, mxu_index=n % 2)
            pltpu.matmul_acc_lhs(acc, act[:, pl.ds(k * MXU, MXU)], load_staged_rhs=k % 2)
        y = pltpu.matmul_pop(acc)
        width = min(MXU, main + pad - n * MXU)
        lane = n * MXU - main if n * MXU >= main else pad + n * MXU
        y = y.reshape(2, half, MXU)[:, :, :width]
        y_buf[layer, :, :, pl.ds(lane, width)] = y
        y_half[layer, :, :, pl.ds(lane, width)] = y.astype(jnp.bfloat16)

    def number_slots(layer):
        for chip in range(chips):
            count = jnp.int32(0)
            for t in range(rows):
                named = route_nums[layer, t, 0] == chip
                for k in range(1, route_nums.shape[2]):
                    named = named | (route_nums[layer, t, k] == chip)
                slots[layer, chip, t] = jnp.where(named, count, -1)
                count = count + jnp.where(named, 1, 0)

    def pack(layer, chip):
        spots = [slots[layer, chip, t] for t in range(rows)]

        def piece(lane, width, j):
            place = lax.broadcasted_iota(jnp.int32, (rows, width), 0)
            value = jnp.zeros((rows, width), jnp.float32)
            for t in range(rows):
                row = jnp.broadcast_to(norm_buf[t : t + 1, pl.ds(lane, width)], (rows, width))
                value = jnp.where(place == spots[t], row, value)
            if j is not None:
                for t in range(rows):
                    row = jnp.broadcast_to(norm_buf[t : t + 1, pl.ds(main, width)], (rows, width))
                    spot = jnp.where(spots[t] == j, CAP, -1)
                    value = jnp.where(place == spot, row, value)
            return value.astype(jnp.bfloat16)

        pieces = [piece(j * pad, pad, j) for j in range(CAP)]
        if CAP * pad < main:
            pieces.append(piece(CAP * pad, main - CAP * pad, None))
        return jnp.concatenate(pieces, axis=1)

    def unfold(value):
        place = lax.rem(lax.broadcasted_iota(jnp.int32, (8, pad), 0), rows)
        total = jnp.zeros((8, pad), jnp.float32)
        for j in range(CAP):
            moved = pltpu.roll(value[:, j * pad : (j + 1) * pad], 8 + j - CAP, 0)
            total = jnp.where(place == j, moved, total)
        return total

    def fold(part, middle, end):
        c0, cw = parts[part]
        place = lax.rem(lax.broadcasted_iota(jnp.int32, (8, pad), 0), rows)
        pieces = []
        lane = 0
        for j in range(CAP):
            if c0 <= j * pad < c0 + cw:
                moved = pltpu.roll(end, CAP - j, 0)
                pieces.append(jnp.where(place == CAP, moved, middle[:, lane : lane + pad]))
                lane += pad
        if lane < cw:
            pieces.append(middle[:, lane:])
        return jnp.concatenate(pieces, axis=1) if len(pieces) > 1 else pieces[0]

    unrolled = chips <= 16 and chips & (chips - 1) == 0

    def mirror(flip):
        total = 0
        bit = 1
        while bit < chips:
            own = lax.rem(me // bit, 2)
            total = total + bit * (1 - own if flip & bit else own)
            bit *= 2
        return total

    mirrored = [mirror(flip) for flip in range(chips - 1, 0, -1)] if unrolled else []

    def each_peer(body):
        for peer in mirrored:
            body(peer)
        if not unrolled:
            @pl.loop(1, chips)
            def _(d):
                body(lax.rem(me + d, chips))

    def near_peers(body):
        for peer in mirrored[::-1]:
            body(peer)
        if not unrolled:
            each_peer(body)

    def each_group(count, body):
        if fast:
            for q in range(count):
                body(q)
        else:
            pl.loop(0, count)(body)

    def each_chip(body):
        if unrolled:
            for slot in range(chips):
                body(slot)
        else:
            pl.loop(0, chips)(body)

    def gather_copy(layer, cut, half_idx, peer, slot):
        block = gathered.at[layer, half_idx, slot, :, pl.ds(*cuts[cut])]
        return pltpu.make_async_remote_copy(
            src_ref=packed.at[layer, peer] if fast else block,
            dst_ref=block,
            send_sem=ag_send.at[layer, cut, peer],
            recv_sem=ag_recv.at[layer, cut, slot],
            device_id={"expert": peer, "dp": other},
            device_id_type=MESH,
        )

    def forward_copy(layer, cut, half_idx, slot):
        block = gathered.at[layer, half_idx, slot, :, pl.ds(*cuts[cut])]
        return pltpu.make_async_remote_copy(
            src_ref=block,
            dst_ref=block,
            send_sem=fw_send.at[layer, cut, slot],
            recv_sem=fw_recv.at[layer, cut, slot],
            device_id={"dp": other},
            device_id_type=MESH,
        )

    def pair_copy(layer, part):
        c0, cw = pair_lanes[part]
        return pltpu.make_async_remote_copy(
            src_ref=y_half.at[layer, core, :, pl.ds(c0, cw)],
            dst_ref=peer_buf.at[layer, :, pl.ds(c0, cw)],
            send_sem=pr_send.at[layer, part],
            recv_sem=pr_recv.at[layer, part],
            device_id={"dp": other},
            device_id_type=MESH,
        )

    def home_copy(layer, part, peer, slot_src, slot_dst):
        c0, cw = parts[part]
        return pltpu.make_async_remote_copy(
            src_ref=blocks.at[layer, slot_src, :, pl.ds(c0, cw)],
            dst_ref=back.at[layer, slot_dst, :, pl.ds(c0, cw)],
            send_sem=rs_send.at[layer, part, peer],
            recv_sem=rs_recv.at[layer, part, slot_dst],
            device_id={"expert": peer, "dp": other},
            device_id_type=MESH,
        )

    def beside_copy(layer, part):
        c0, cw = parts[part]
        return pltpu.make_async_remote_copy(
            src_ref=blocks.at[layer, me, :, pl.ds(c0, cw)],
            dst_ref=back.at[layer, me, :, pl.ds(c0, cw)],
            send_sem=rs_send.at[layer, part, me],
            recv_sem=rs_recv.at[layer, part, me],
            device_id={"dp": other},
            device_id_type=MESH,
        )

    inputs = [
        pltpu.make_async_copy(src, dst, in_sem.at[i])
        for i, (src, dst) in enumerate(
            ((tok_hbm, tok_ref), (gain_hbm, gain_ref), (routes_hbm, routes_ref), (gates_hbm, gates_ref))
        )
    ]
    if fast:
        inputs.append(pltpu.make_async_copy(routes_hbm, route_nums, in_sem.at[4]))
    for copy in inputs:
        copy.start()
    barrier = pltpu.get_barrier_semaphore()
    each_peer(
        lambda peer: pl.semaphore_signal(
            barrier, inc=1, device_id={"expert": peer, "dp": other}, device_id_type=MESH
        )
    )
    pl.semaphore_signal(barrier, inc=1, device_id={"dp": other}, device_id_type=MESH)
    for copy in inputs:
        copy.wait()
    for copy in weights(0):
        copy.start()

    if fast:
        number_slots(0)
        norm_buf[...] = jnp.zeros_like(norm_buf)
    hidden[...] = tok_ref[...].astype(jnp.float32)
    gains = gain_ref[...].astype(jnp.float32)
    for layer in range(layers):
        x = hidden[...]
        scale_inv = lax.rsqrt(jnp.mean(x * x, axis=-1, keepdims=True) + EPS)
        normed = (x * scale_inv * gains[layer : layer + 1]).astype(jnp.bfloat16)
        if fast:
            norm_buf[:, pl.ds(0, d_model)] = normed.astype(jnp.float32)
        else:
            gathered[layer, core, me] = normed
        if layer == 0:
            if fast:
                for peer in mirrored:
                    packed[layer, peer] = pack(layer, peer)
                gathered[layer, core, me] = pack(layer, me)
            pl.semaphore_wait(barrier, chips)
        for cut in range(len(cuts)):
            def hand_out(peer):
                if fast and layer > 0:
                    packed[layer, peer] = pack(layer, peer)
                gather_copy(layer, cut, core, peer, me).start()

            each_peer(hand_out)
            if fast and layer > 0:
                gathered[layer, core, me] = pack(layer, me)
            forward_copy(layer, cut, core, me).start()
        if fast and layer + 1 < layers:
            number_slots(layer + 1)
        if layer == 0:
            for later in range(1, layers):
                for copy in weights(later):
                    copy.start()
        if fast:
            turn_all(layer, [(i, f) for f in range(strips) for i in range(2) if layer == 0 or i == 1])
            pad_down(layer)

        for cut in range(len(cuts)):
            def pass_on(peer):
                gather_copy(layer, cut, other, peer, peer).wait_recv()
                forward_copy(layer, cut, other, peer).start()

            near_peers(pass_on)

        per = 8 // rows

        def stack(cut):
            c0, cw = cuts[cut]
            cols = pl.ds(c0, cw)
            def lift(h):
                whole_rows, end_rows = [], []

                def one_group(q):
                    value = jnp.concatenate(
                        [
                            gathered[layer, h, q * per + i, :, cols].astype(jnp.float32)
                            for i in range(per)
                        ],
                        axis=0,
                    )
                    if fast:
                        whole_rows.append(value)
                        end_rows.append(unfold(value))
                    else:
                        stacked[h, q, :, cols] = value

                each_group(chips // per, one_group)
                if fast:
                    height = pl.ds(pl.multiple_of(h * half, half), half)
                    for lanes, found in ((cols, whole_rows), (pl.ds(main, pad), end_rows)):
                        x_buf[height, lanes] = jnp.concatenate(found, axis=0).astype(jnp.bfloat16)

            forward_copy(layer, cut, other, me).wait_recv()
            if fast:
                lift(other)
            each_peer(lambda peer: forward_copy(layer, cut, core, peer).wait_recv())
            if fast:
                lift(core)
            else:
                lift(0)
                lift(1)
                x_buf[:, cols] = stacked[:, :, :, cols].reshape(2 * half, cw).astype(jnp.bfloat16)

        if fast:
            short = x_buf.shape[1] - main - pad
            if short and layer == 0:
                x_buf[:, pl.ds(main + pad, short)] = jnp.zeros((2 * half, short), jnp.bfloat16)
        else:
            for cut in range(len(cuts)):
                stack(cut)
            w_gate, w_up, w_down = weights(layer)
            w_gate.wait()
            w_up.wait()

        def up_tile(c0, cw):
            cols = pl.ds(c0, cw)
            g = dot_rows(wg[layer, cols, :], x_buf[...]).T
            u = dot_rows(wu[layer, cols, :], x_buf[...]).T
            act[:, cols] = (g * jax.nn.sigmoid(1.702 * g) * (u + 1.0)).astype(jnp.bfloat16)

        if fast:
            for cut, (c0, cw) in enumerate(cuts):
                stack(cut)
                multiply_up(layer, range(-(-d_model // MXU)), True)
            down_copy(layer).wait()
        else:
            tiled_loop(0, ff, TILE, up_tile)
            w_down.wait()

        def down_tile(c0, cw):
            cols = pl.ds(c0, cw)
            y = jnp.dot(act[...], wd[layer, :, cols], preferred_element_type=jnp.float32)
            y_buf[layer, :, :, cols] = y.reshape(2, half, cw)
            y_half[layer, :, :, cols] = y.reshape(2, half, cw).astype(jnp.bfloat16)

        def send_home(part):
            c0, cw = parts[part]
            cols = pl.ds(c0, cw)
            pair_copy(layer, part).wait_recv()

            def one_group(q):
                group = pl.ds(q * 8 if fast else pl.multiple_of(q * 8, 8), 8)
                def added(lanes):
                    mine, theirs = y_buf[layer, other, group, lanes], peer_buf[layer, group, lanes]
                    return mine + theirs.astype(jnp.float32)

                if fast:
                    total = fold(part, added(pl.ds(pad + c0, cw)), added(pl.ds(0, pad)))
                else:
                    total = added(cols)
                for i in range(per):
                    blocks[layer, q * per + i, :, cols] = total[i * rows : (i + 1) * rows].astype(
                        jnp.bfloat16
                    )

            each_group(chips // per, one_group)
            each_peer(lambda peer: home_copy(layer, part, peer, peer, me).start())
            beside_copy(layer, part).start()

        for part, (c0, cw) in enumerate(parts):
            if fast:
                first = range(main // MXU, -(-d_model // MXU)) if part == 0 else ()
                for n in (*first, *range(c0 // MXU, (c0 + cw) // MXU)):
                    multiply_down(layer, n)
            else:
                tiled_loop(c0, c0 + cw, TILE, down_tile)
            pair_copy(layer, part).start()
            if part > 0 and not fast:
                send_home(part - 1)
        for part in range(len(parts)) if fast else [len(parts) - 1]:
            send_home(part)
        if fast and layer + 1 < layers:
            turn_all(layer + 1, [(0, f) for f in range(strips)])

        routes = routes_ref[layer]
        gates = gates_ref[layer]

        def weight_of(chip):
            expert = chip // chips_per_expert
            return jnp.sum(jnp.where(routes == expert, gates, 0.0), axis=1, keepdims=True)

        def shares_of(chip):
            place = lax.broadcasted_iota(jnp.int32, (rows, 1), 0)
            spot = jnp.full((rows, 1), -1, jnp.int32)
            for t in range(rows):
                spot = jnp.where(place == t, slots[layer, chip, t], spot)
            weight = weight_of(chip)
            return [jnp.where(spot == j, weight, 0.0) for j in range(CAP)]

        def add(chip, shares):
            if not fast:
                hidden[...] += weight_of(chip) * back[layer, chip].astype(jnp.float32)
                return
            block = back[layer, chip].astype(jnp.float32)
            middle = sum(shares[j] * block[j : j + 1] for j in range(CAP))
            end = sum(shares[j] * block[CAP : CAP + 1, j * pad : (j + 1) * pad] for j in range(CAP))
            hidden[:, pl.ds(0, main)] += middle
            hidden[:, pl.ds(main, d_model - main)] += end[:, : d_model - main]

        def take(peer, shares=None):
            for part in range(len(parts)):
                home_copy(layer, part, peer, peer, peer).wait_recv()
            add(peer, shares)

        own = shares_of(me) if fast else None
        known = [shares_of(peer) for peer in mirrored[::-1]] if fast else []
        for part in range(len(parts)):
            beside_copy(layer, part).wait_recv()
        add(me, own)
        if fast:
            for peer, shares in zip(mirrored[::-1], known):
                take(peer, shares)
        else:
            near_peers(take)
        result = hidden[...].astype(jnp.bfloat16)
        if layer + 1 < layers:
            hidden[...] = result.astype(jnp.float32)
        else:
            out_ref[...] = result

    for layer in range(layers):
        for cut in range(len(cuts)):
            each_peer(lambda peer: forward_copy(layer, cut, other, peer).wait_send())
            forward_copy(layer, cut, core, me).wait_send()

        def sent(peer):
            for cut in range(len(cuts)):
                gather_copy(layer, cut, core, peer, me).wait_send()
            for part in range(len(parts)):
                home_copy(layer, part, peer, peer, me).wait_send()

        each_peer(sent)
        for part in range(len(parts)):
            pair_copy(layer, part).wait_send()
            beside_copy(layer, part).wait_send()


def on_device(tokens, norm_gain, w_gate, w_up, w_down, routes, gates, *, expert_total_of):
    chips = lax.axis_size("expert")
    cores = lax.axis_size("dp")
    rows, d_model = tokens.shape
    layers, _, ff = w_gate.shape
    expert_total = expert_total_of(d_model, ff, chips * cores)
    half = chips * rows
    vmem = pl.BlockSpec(memory_space=pltpu.VMEM)
    top = routes.shape[-1]
    hbm = pl.BlockSpec(memory_space=pl.ANY)
    dma = pltpu.SemaphoreType.DMA
    parts = len(col_tiles(0, d_model, -(-d_model // (128 * PARTS)) * 128))
    bf16, f32 = jnp.bfloat16, jnp.float32
    fast = tiled(chips, chips // expert_total, rows, d_model, ff)
    main, pad = folded(d_model) if fast else (d_model, 0)
    lanes = main + pad
    strips = -(-ff // MXU)
    whole, high = d_model // MXU * MXU, strips * MXU
    rest, wide = d_model - whole, -(-d_model // MXU) * MXU
    body = functools.partial(kernel, chips, chips // expert_total)
    if fast:
        ups = [pltpu.VMEM((layers, high, whole), bf16)] * 2 + [pltpu.VMEM((layers, ff, whole), bf16)]
        tails = [pltpu.VMEM((layers, high, rest), bf16)] * 3
        tails += [pltpu.VMEM((layers, rest, high), bf16)] * 2 + [pltpu.VMEM((layers, high, MXU), bf16)]
        tails += [
            pltpu.VMEM((layers, chips, rows, main), bf16),
            pltpu.VMEM((rows, lanes), f32),
            pltpu.SMEM((layers, rows, top), jnp.int32),
            pltpu.SMEM((layers, chips, rows), jnp.int32),
        ]
        x_shape, act_shape, w_sems = (2 * half, wide), (2 * half, high), (layers, 3, strips + 1)

        def body(*refs):
            each = [pltpu.ACC(i)((2 * half, MXU), f32) for i in range(2) for _ in range(strips)]
            pl.run_scoped(
                lambda *accs: kernel(
                    chips, chips // expert_total, *refs, accs=(accs[:strips], accs[strips:])
                ),
                *each,
            )
    else:
        ups, tails = [pltpu.VMEM((layers, ff, d_model), bf16)] * 3, []
        x_shape, act_shape, w_sems = (2 * half, d_model), (2 * half, ff), (layers, 3)
    return pl.pallas_call(
        body,
        out_shape=jax.ShapeDtypeStruct(tokens.shape, tokens.dtype),
        in_specs=[hbm] * 7,
        out_specs=vmem,
        scratch_shapes=[
            *ups,
            pltpu.VMEM((layers, 2, chips, rows, main), bf16),
            pltpu.VMEM((2, half // 8, 8, lanes), f32),
            pltpu.VMEM(x_shape, bf16),
            pltpu.VMEM(act_shape, bf16),
            pltpu.VMEM((layers, 2, half, lanes), f32),
            pltpu.VMEM((layers, 2, half, lanes), bf16),
            pltpu.VMEM((layers, half, lanes), bf16),
            pltpu.VMEM((layers, chips, rows, main), bf16),
            pltpu.VMEM((layers, chips, rows, main), bf16),
            pltpu.VMEM((rows, d_model), f32),
            dma(w_sems),
            dma((layers, CUTS, chips)),
            dma((layers, CUTS, chips)),
            dma((layers, CUTS, chips)),
            dma((layers, CUTS, chips)),
            dma((layers, parts)),
            dma((layers, parts)),
            dma((layers, parts, chips)),
            dma((layers, parts, chips)),
            pltpu.VMEM((rows, d_model), bf16),
            pltpu.VMEM((layers, d_model), bf16),
            pltpu.VMEM((layers, rows, top), jnp.int32),
            pltpu.VMEM((layers, rows, top), f32),
            dma((5,)),
            *tails,
        ],
        compiler_params=pltpu.CompilerParams(
            collective_id=0, has_side_effects=True, vmem_limit_bytes=67043328
        ),
    )(
        tokens,
        norm_gain,
        jnp.swapaxes(w_gate, 1, 2),
        jnp.swapaxes(w_up, 1, 2),
        w_down,
        routes,
        gates,
    )


def solution(mesh):
    def expert_total_of(d_model, ff, devices):
        return devices * ff // d_model

    return jax.shard_map(
        functools.partial(on_device, expert_total_of=expert_total_of),
        mesh=mesh,
        in_specs=(
            P(("groups", "expert", "dp"), None),
            P(),
            P(None, None, ("expert", "dp")),
            P(None, None, ("expert", "dp")),
            P(None, ("expert", "dp"), None),
            P(None, ("groups", "expert", "dp"), None),
            P(None, ("groups", "expert", "dp"), None),
        ),
        out_specs=P(("groups", "expert", "dp"), None),
        check_vma=False,
    )
```
